32 devices in a mesh: rep: 16 (over z, x, core), tp: 2 (over y).
Axes of the slice: x: 2, y: 2, z: 4, core: 2. Of those that a mesh axis runs over, the one named last changes fastest.
Arguments:
- images: bfloat16 [32768, 1024], P(('rep', 'tp')), may hold values from -6 to 6
- labels: int32 [128], P('rep'), may hold values from 0 to 999
- first_weight: bfloat16 [16384, 4096], P('rep', 'tp'), may hold values from -0.1875 to 0.1875
- second_weight: bfloat16 [65536, 1024], P(('rep', 'tp')), may hold values from -0.09375 to 0.09375
- head_weight: bfloat16 [16384, 1000], P('rep', 'tp'), may hold values from -0.1875 to 0.1875
- push_weights: float32 [16], P('rep'), may hold values from 0.5 to 2
- round_index: int32 [1], replicated, may hold values from 0 to 2
- lr_first: float32 [1], replicated, may hold values from 10 to 40
- lr_second: float32 [1], replicated, may hold values from 1 to 4
- lr_head: float32 [1], replicated, may hold values from 0.1 to 0.5
Outputs:
- new_first: bfloat16 [16384, 4096], P('rep', 'tp')
- new_second: bfloat16 [65536, 1024], P(('rep', 'tp'))
- new_head: bfloat16 [16384, 1000], P('rep', 'tp')
- new_mass: float32 [16], P('rep')
The draws below stay inside these ranges and needn't reach their ends.
Inputs may be any that keep to these rules, and one draw needn't show every extreme that they name: `round_index`: k picks the peers at offsets 2^k and 2^(k+1) among the 16 replicas.
All inputs are finite; a program needn't handle non-finite values.
Results may differ from the reference program's by a relative error of at most 0.0056.
The reference program's roundings to bfloat16 on the way (of `normed` and `dpre`) count: a program that leaves them out, or rounds other values in their place, can miss the bound.
Values may be sent and summed in bfloat16 or wider, within the bound.
A program may use at most 128 MiB of HBM per device.

```python
import math
from functools import partial
import jax
import jax.numpy as jnp
from jax import lax

D = 1024
FF = 4096
CLASSES = 1000
SEQ = 256
IMG = 8
N_REP = 16


def touch_ends(values, stream_key, smallest, top_value):
    longest = values.shape.index(max(values.shape))
    spots = []
    for shift in (0, 1):
        where = [jax.random.randint(jax.random.fold_in(stream_key, axis), (), 0, length) for axis, length in enumerate(values.shape)]
        where[longest] = (where[longest] + shift) % values.shape[longest]
        spots.append(tuple(where))
    return values.at[spots[0]].set(smallest).at[spots[1]].set(top_value)


def shard_levels(own_key, dims, pieces, low, high):
    loudness = 1.0
    for axis_at, shards_of in pieces:
        steps = jax.random.uniform(jax.random.fold_in(jax.random.fold_in(own_key, 6), axis_at), (shards_of,), jnp.float32, low / len(pieces), high / len(pieces))
        loudness = loudness * jnp.repeat(jnp.exp(steps), dims[axis_at] // shards_of).reshape((-1,) + (1,) * (len(dims) - 1 - axis_at))
    return loudness


def scatter_about(key, extent, width, limit, cuts=(), kind=jnp.bfloat16):
    factor_of = shard_levels(key, extent, cuts, -0.22, 0.18) if cuts else 1.0
    values = jax.random.normal(key, extent, jnp.float32) * width * factor_of
    return jnp.minimum(jnp.maximum(values, -limit), limit).astype(kind)


def setup_inputs(seed: int = 0) -> dict:
    seeds = jax.random.split(jax.random.key(seed), 11)
    images = scatter_about(seeds[0], (N_REP * IMG * SEQ, D), 1.0, 6.0, ((0, 32),))
    labels = touch_ends(jax.random.randint(seeds[1], (N_REP * IMG,), 0, CLASSES), jax.random.fold_in(seeds[1], 1), 0, CLASSES - 1).astype(jnp.int32)
    first_weight = scatter_about(seeds[2], (N_REP * D, FF), D ** -0.5, 0.1875, ((0, 16), (1, 2)))
    second_weight = scatter_about(seeds[3], (N_REP * FF, D), FF ** -0.5, 0.09375, ((0, 32),))
    head_weight = scatter_about(seeds[4], (N_REP * D, CLASSES), D ** -0.5, 0.1875, ((0, 16), (1, 2)))
    push_weights = jnp.clip(jnp.exp(math.log(2.0) - 1.3862944 * jax.random.uniform(seeds[5], (N_REP,), jnp.float32) ** shard_levels(seeds[5], (N_REP,), ((0, 16),), -0.2, 0.2)), 0.5, 2.0)
    round_index = jax.random.randint(seeds[6], (1,), 0, 3).astype(jnp.int32)
    lr_first = jnp.clip(jnp.exp(jax.random.uniform(seeds[7], (1,), jnp.float32, math.log(10.0), math.log(40.0))), 10.0, 40.0)
    lr_second = jnp.clip(jnp.exp(jax.random.uniform(seeds[8], (1,), jnp.float32, math.log(1.0), math.log(4.0))), 1.0, 4.0)
    lr_head = jnp.clip(jnp.exp(jax.random.uniform(seeds[9], (1,), jnp.float32, math.log(0.1), math.log(0.5))), 0.1, 0.5)
    return {"images": images, "labels": labels, "first_weight": first_weight, "second_weight": second_weight, "head_weight": head_weight, "push_weights": push_weights, "round_index": round_index, "lr_first": lr_first, "lr_second": lr_second, "lr_head": lr_head}


COEF = 0.7978845608
CUBIC = 0.044715
HIGH = lax.Precision.HIGHEST

def normalize(rows):
    values = rows.astype(jnp.float32)
    center = values - lax.optimization_barrier(jnp.mean(values, axis=-1, keepdims=True))
    spread = lax.optimization_barrier(jnp.mean(center * center, axis=-1, keepdims=True))
    return (center * lax.rsqrt(spread + 1e-05)).astype(jnp.bfloat16)

def gelu_pair(pre):
    tanh_val = jnp.tanh(COEF * (pre + CUBIC * pre * pre * pre))
    value = 0.5 * pre * (1.0 + tanh_val)
    slope = 0.5 * (1.0 + tanh_val) + 0.5 * pre * (1.0 - tanh_val * tanh_val) * COEF * (1.0 + 3.0 * CUBIC * pre * pre)
    return (value, slope)

def replica_step(packed, lr_first, lr_second, lr_head):
    tokens, classes, first, second, head, mass = packed
    z_first = (first.astype(jnp.float32) / mass).astype(jnp.bfloat16)
    z_second = (second.astype(jnp.float32) / mass).astype(jnp.bfloat16)
    z_head = (head.astype(jnp.float32) / mass).astype(jnp.bfloat16)
    normed = normalize(tokens)
    pre = jnp.dot(normed, z_first, preferred_element_type=jnp.float32)
    act, slope = gelu_pair(pre)
    mean_act = lax.optimization_barrier(jnp.mean(act.reshape(IMG, SEQ, FF), axis=1))
    mean_tok = lax.optimization_barrier(jnp.mean(tokens.astype(jnp.float32).reshape(IMG, SEQ, D), axis=1))
    second_f = z_second.astype(jnp.float32)
    pooled = mean_tok + jnp.dot(mean_act, second_f, precision=HIGH)
    pooled_b = pooled.astype(jnp.bfloat16)
    logits = jnp.dot(pooled_b, z_head, preferred_element_type=jnp.float32)
    expo = jnp.exp(logits)
    prob = expo / lax.optimization_barrier(jnp.sum(expo, axis=1, keepdims=True))
    onehot = (classes[:, None] == jnp.arange(CLASSES, dtype=jnp.int32)[None, :]).astype(jnp.float32)
    dlog = (prob - onehot) / IMG
    grad_head = jnp.dot(pooled_b.astype(jnp.float32).T, dlog, precision=HIGH)
    dpool = jnp.dot(dlog, z_head.astype(jnp.float32).T, precision=HIGH)
    dmean = jnp.dot(dpool, second_f.T, precision=HIGH)
    grad_second = jnp.dot(mean_act.T, dpool, precision=HIGH)
    dpre = (dmean[:, None, :] / SEQ * slope.reshape(IMG, SEQ, FF)).reshape(IMG * SEQ, FF).astype(jnp.bfloat16)
    grad_first = jnp.dot(normed.T, dpre, preferred_element_type=jnp.float32)
    sent_first = (first.astype(jnp.float32) - lr_first * grad_first).astype(jnp.bfloat16)
    sent_second = (second.astype(jnp.float32) - lr_second * grad_second).astype(jnp.bfloat16)
    sent_head = (head.astype(jnp.float32) - lr_head * grad_head).astype(jnp.bfloat16)
    sent_mass = mass.astype(jnp.bfloat16)
    return (sent_first, sent_second, sent_head, sent_mass)

def reference(images, labels, first_weight, second_weight, head_weight, push_weights, round_index, lr_first, lr_second, lr_head):
    packed = (images.reshape(N_REP, IMG * SEQ, D), labels.reshape(N_REP, IMG), first_weight.reshape(N_REP, D, FF), second_weight.reshape(N_REP, FF, D), head_weight.reshape(N_REP, D, CLASSES), push_weights)
    step_fn = partial(replica_step, lr_first=lr_first[0], lr_second=lr_second[0], lr_head=lr_head[0])
    sent_first, sent_second, sent_head, sent_mass = lax.map(step_fn, packed)
    near_off = jnp.left_shift(jnp.int32(1), round_index[0])
    far_off = near_off * 2

    def spread(stack):
        values = stack.astype(jnp.float32)
        return (values + jnp.roll(values, near_off, axis=0) + jnp.roll(values, far_off, axis=0)) / 3.0
    new_first = spread(sent_first).astype(jnp.bfloat16).reshape(N_REP * D, FF)
    new_second = spread(sent_second).astype(jnp.bfloat16).reshape(N_REP * FF, D)
    new_head = spread(sent_head).astype(jnp.bfloat16).reshape(N_REP * D, CLASSES)
    new_mass = spread(sent_mass)
    return (new_first, new_second, new_head, new_mass)
```

```python
from functools import partial

import jax
import jax.numpy as jnp
from jax import lax
from jax.sharding import PartitionSpec as P

SEQ = 256
IMG = 8
CHUNKS = 4
LEVELS = 3

COEF = 0.7978845608
CUBIC = 0.044715


def shifted(value, axis, by):
    peers = lax.axis_size(axis)
    return lax.ppermute(value, axis, [(i, (i + by) % peers) for i in range(peers)])


def swapped(value, axis, bit):
    peers = lax.axis_size(axis)
    return lax.ppermute(value, axis, [(i, i ^ bit) for i in range(peers)])


def pull(value, near):
    peers = lax.axis_size("rep")
    if near <= 2 and peers % (2 * near) == 0:
        far_in = shifted(value, "rep", 2 * near)
        has_bit = (lax.axis_index("rep") & near) != 0
        near_in = swapped(jnp.where(has_bit, far_in, value), "rep", near)
        return near_in, far_in
    near_in = shifted(value, "rep", near)
    return near_in, shifted(near_in, "rep", near)


def tp_sum(value):
    if lax.axis_size("tp") == 2:
        return value + swapped(value, "tp", 1)
    return lax.psum(value, "tp")


def normalize(rows):
    values = rows.astype(jnp.float32)
    center = values - jnp.mean(values, axis=-1, keepdims=True)
    spread = jnp.mean(center * center, axis=-1, keepdims=True)
    return (center * lax.rsqrt(spread + 1e-05)).astype(jnp.bfloat16)


def gelu_pair(pre):
    tanh_val = jnp.tanh(COEF * (pre + CUBIC * pre * pre * pre))
    value = 0.5 * pre * (1.0 + tanh_val)
    slope = 0.5 * (1.0 + tanh_val) + 0.5 * pre * (1.0 - tanh_val * tanh_val) * COEF * (
        1.0 + 3.0 * CUBIC * pre * pre
    )
    return (value, slope)


def pieces(value):
    high = lax.reduce_precision(value, 8, 7)
    rest = value - high
    middle = lax.reduce_precision(rest, 8, 7)
    return [part.astype(jnp.bfloat16) for part in (high, middle, rest - middle)]


def few_rows_dot(rows, weight, weight_dim):
    count = rows.shape[0]
    stack = jnp.concatenate(pieces(rows), axis=0)
    out = lax.dot_general(
        stack, weight, (((1,), (weight_dim,)), ((), ())), preferred_element_type=jnp.float32
    )
    return out[:count] + (out[count : 2 * count] + out[2 * count :])


def outer_sum(left, right):
    a, b, c = pieces(left)
    x, y, z = pieces(right)
    return lax.dot_general(
        jnp.concatenate([a, a, b, b, a, c], axis=0),
        jnp.concatenate([x, y, x, y, z, x], axis=0),
        (((0,), (0,)), ((), ())),
        preferred_element_type=jnp.float32,
    )


def mean_of_three(own, near_in, far_in):
    return (
        own.astype(jnp.float32) + near_in.astype(jnp.float32) + far_in.astype(jnp.float32)
    ) / 3.0


def round_of(
    level,
    images,
    labels,
    first_weight,
    second_weight,
    head_weight,
    push_weights,
    lr_first,
    lr_second,
    lr_head,
):
    near = 1 << level
    tp_size = lax.axis_size("tp")
    tp_at = lax.axis_index("tp")
    local_rows = images.shape[0]
    width = images.shape[1]
    class_local = head_weight.shape[1]
    hidden_local = first_weight.shape[1]

    near_second, far_second = pull(second_weight, near)
    near_head, far_head = pull(head_weight, near)

    mass = push_weights[0]
    normed_local = normalize(images)
    in_pairs = tp_size == 2 and local_rows % SEQ == 0
    if in_pairs:
        blocks = [normed_local, swapped(normed_local, "tp", 1)]
    else:
        blocks = [lax.all_gather(normed_local, "tp", axis=0, tiled=True)]
    z_first = (first_weight.astype(jnp.float32) / mass).astype(jnp.bfloat16)
    z_second = (second_weight.astype(jnp.float32) / mass).astype(jnp.bfloat16)
    z_head = (head_weight.astype(jnp.float32) / mass).astype(jnp.bfloat16)

    means, slopes = [], []
    for block in blocks:
        pre = jnp.dot(block, z_first, preferred_element_type=jnp.float32)
        act, slope = gelu_pair(pre)
        means.append(jnp.mean(act.reshape(-1, SEQ, hidden_local), axis=1))
        slopes.append(slope.reshape(-1, SEQ, hidden_local))

    def in_order(parts):
        if len(parts) == 1:
            return parts[0]
        return jnp.where(
            tp_at == 0, jnp.concatenate(parts, axis=0), jnp.concatenate(parts[::-1], axis=0)
        )

    mean_act = in_order(means)
    row_start = tp_at * local_rows
    if in_pairs:
        own_tok = jnp.mean(images.astype(jnp.float32).reshape(-1, SEQ, width), axis=1)
        mean_tok = in_order([own_tok, jnp.zeros_like(own_tok)])
    else:
        image_of = (row_start + jnp.arange(local_rows, dtype=jnp.int32)) // SEQ
        picker = (image_of[None, :] == jnp.arange(IMG, dtype=jnp.int32)[:, None]).astype(
            jnp.bfloat16
        )
        mean_tok = jnp.dot(picker, images, preferred_element_type=jnp.float32) / SEQ
    pooled = tp_sum(mean_tok + few_rows_dot(mean_act, z_second, 0))
    pooled_b = pooled.astype(jnp.bfloat16)
    logits = jnp.dot(pooled_b, z_head, preferred_element_type=jnp.float32)
    expo = jnp.exp(logits)
    total = tp_sum(jnp.broadcast_to(jnp.sum(expo, axis=1, keepdims=True), (IMG, 128)))[:, :1]
    prob = expo / total
    class_ids = tp_at * class_local + jnp.arange(class_local, dtype=jnp.int32)
    onehot = (labels[:, None] == class_ids[None, :]).astype(jnp.float32)
    dlog = (prob - onehot) / IMG
    dpool = tp_sum(few_rows_dot(dlog, z_head, 1))
    dmean = few_rows_dot(dpool, z_second, 1) / SEQ

    sent_mass = lax.reduce_precision(push_weights, 8, 7)
    own_small = jnp.concatenate(
        [
            mean_act,
            dpool,
            pooled_b.astype(jnp.float32),
            dlog,
            jnp.broadcast_to(sent_mass[None, :], (IMG, 128)),
        ],
        axis=1,
    )
    near_small, far_small = pull(own_small, near)

    if in_pairs:
        half = IMG // 2
        flip = jnp.concatenate([dmean[half:], dmean[:half]], axis=0)
        ordered = jnp.where(tp_at == 0, dmean, flip)
        dmeans = [ordered[:half], ordered[half:]]
    else:
        dmeans = [dmean]
    dpres = [
        (grad[:, None, :] * slope).reshape(-1, hidden_local).astype(jnp.bfloat16)
        for grad, slope in zip(dmeans, slopes)
    ]

    new_first = []
    step = width // CHUNKS
    for chunk in range(CHUNKS):
        rows = slice(chunk * step, (chunk + 1) * step)
        grad_first = sum(
            lax.dot_general(
                block[:, rows],
                dpre,
                (((0,), (0,)), ((), ())),
                preferred_element_type=jnp.float32,
            )
            for block, dpre in zip(blocks, dpres)
        )
        sent = (first_weight[rows].astype(jnp.float32) - lr_first[0] * grad_first).astype(
            jnp.bfloat16
        )
        near_in, far_in = pull(sent, near)
        new_first.append(mean_of_three(sent, near_in, far_in).astype(jnp.bfloat16))
    new_first = jnp.concatenate(new_first, axis=0)

    small = jnp.concatenate([own_small, near_small, far_small], axis=0)
    cut = [hidden_local, hidden_local + width, hidden_local + 2 * width]
    all_act, all_dpool = small[:, : cut[0]], small[:, cut[0] : cut[1]]
    all_pooled, all_dlog = small[:, cut[1] : cut[2]], small[:, cut[2] : cut[2] + class_local]
    new_second = (
        mean_of_three(second_weight, near_second, far_second)
        - (lr_second[0] / 3.0) * outer_sum(all_act, all_dpool)
    ).astype(jnp.bfloat16)
    new_head = (
        mean_of_three(head_weight, near_head, far_head)
        - (lr_head[0] / 3.0) * outer_sum(all_pooled, all_dlog)
    ).astype(jnp.bfloat16)
    last = small.shape[1] - 1
    new_mass = mean_of_three(own_small[:1, last], near_small[:1, last], far_small[:1, last])
    return (new_first, new_second, new_head, new_mass)


def local(
    images,
    labels,
    first_weight,
    second_weight,
    head_weight,
    push_weights,
    round_index,
    lr_first,
    lr_second,
    lr_head,
):
    level = jnp.clip(round_index[0], 0, LEVELS - 1)
    return lax.switch(
        level,
        [partial(round_of, step) for step in range(LEVELS)],
        images,
        labels,
        first_weight,
        second_weight,
        head_weight,
        push_weights,
        lr_first,
        lr_second,
        lr_head,
    )


def solution(mesh):
    return jax.shard_map(
        local,
        mesh=mesh,
        in_specs=(
            P(("rep", "tp"), None),
            P("rep"),
            P("rep", "tp"),
            P(("rep", "tp"), None),
            P("rep", "tp"),
            P("rep"),
            P(),
            P(),
            P(),
            P(),
        ),
        out_specs=(P("rep", "tp"), P(("rep", "tp"), None), P("rep", "tp"), P("rep")),
        check_vma=False,
    )
```
